256 devices in a mesh: rep: 32 (over y_hi, z, core), tp: 8 (over y_lo, x).
Axes of the slice: x: 4, y: 4 (y_hi: 2, y_lo: 2; y = y_hi * 2 + y_lo), z: 8, core: 2. Of those that a mesh axis runs over, the one named last changes fastest.
Arguments:
- queries: bfloat16 [8192, 8192], P('rep', 'tp'), may hold values from -8 to 8
- cand_keys: bfloat16 [8192, 1024], P('rep', 'tp'), may hold values from -6 to 6
- cand_values: bfloat16 [8192, 1024], P('rep', 'tp'), may hold values from -6 to 6
- prefix_kv: bfloat16 [32, 2, 4096, 1024], P('rep', None, None, 'tp'), may hold values from -8 to 8
- owner: int32 [1], replicated, may hold values from 0 to 31
- lengths: int32 [32, 2], P('rep'), may hold values from 1 to 128, as said below
- out_weight: bfloat16 [8192, 4096], P('tp'), may hold values from -2.390625 to 2.390625
Outputs:
- attn_out: bfloat16 [8192, 4096], P(('rep', 'tp'))
The draws below stay inside these ranges and needn't reach their ends.
Inputs may be any that keep to these rules, and one draw needn't show every extreme that they name: Only the slice of prefix_kv at index owner[0] is read. Candidate c of group g has its real tokens in its first lengths[g, c] slots; the rest are padding.
All inputs are finite; a program needn't handle non-finite values.
Results may differ from the reference program's by a relative error of at most 0.017.
Values may be sent and summed in bfloat16 or wider, within the bound.
No kernel may reach another device: no remote copies, remote signals or barrier semaphores. Data moves between devices by JAX's collectives and lax.ppermute only.
A program may use at most 64 MiB of HBM per device.

```python
import math
import jax
import jax.numpy as jnp
from jax import lax

QH = 64
KVH = 8
HD = 128
DWIN = 4096
PREFIX = 4096
CLEN = 128
CANDS = 2
GROUPS = 32
ROWS = 256
TOTAL_ROWS = 8192
N_TP = 8


def draw_queries(key, part):
    array_shape = (TOTAL_ROWS, QH * HD)
    values = jnp.clip(jax.random.normal(jax.random.fold_in(key, 1), array_shape, jnp.float32), -6.0, 6.0)
    return values.astype(jnp.bfloat16)


def draw_prefix_kv(key, part):
    array_shape = (GROUPS, 2, PREFIX, KVH * HD)
    values = jnp.clip(jax.random.normal(jax.random.fold_in(key, 2), array_shape, jnp.float32), -6.0, 6.0)
    return values.astype(jnp.bfloat16)


def draw_lengths(key, part):
    counts = jax.random.randint(jax.random.fold_in(key, 3), (GROUPS * CANDS,), 1, CLEN + 1, dtype=jnp.int32)
    chosen = jax.random.randint(jax.random.fold_in(key, 4), (), 0, GROUPS * CANDS, dtype=jnp.int32)
    counts = counts.at[chosen].set(CLEN)
    return counts.reshape(GROUPS, CANDS)


def levels(key, shape, split, least, top_value):
    gain, own = 1.0, jax.random.fold_in(key, 6)
    for dim, shards_of in split:
        steps = jnp.exp(jax.random.uniform(jax.random.fold_in(own, dim), (shards_of,), jnp.float32, least / len(split), top_value / len(split)))
        gain = gain * jnp.repeat(steps, shape[dim] // shards_of).reshape([-1 if axis == dim else 1 for axis in range(len(shape))])
    return gain


def normal_values(own_key, shape, spread, limit, cuts=(), kind=jnp.bfloat16):
    values = spread * jax.random.normal(own_key, shape, jnp.float32)
    if cuts:
        values = values * levels(own_key, shape, cuts, -0.22, 0.18)
    return jnp.clip(values, -limit, limit).astype(kind)


def setup_inputs(seed: int = 0) -> dict:
    key_of = jax.random.split(jax.random.key(seed), 8)
    return {
        "queries": draw_queries(jax.random.fold_in(key_of[7], 71), 0),
        "cand_keys": normal_values(key_of[1], (TOTAL_ROWS, KVH * HD), 1.0, 6.0, ((0, 32), (1, 8))),
        "cand_values": normal_values(key_of[2], (TOTAL_ROWS, KVH * HD), 1.0, 6.0, ((0, 32), (1, 8))),
        "prefix_kv": draw_prefix_kv(jax.random.fold_in(key_of[7], 71), 0),
        "owner": jax.random.randint(key_of[4], (1,), 0, GROUPS).astype(jnp.int32),
        "lengths": draw_lengths(jax.random.fold_in(key_of[7], 71), 0),
        "out_weight": normal_values(key_of[6], (QH * HD, DWIN), 0.4, 2.390625, ((0, 8),)),
    }


NEG = -1e+30

def group_context(inputs, prefix_keys, prefix_values):
    group_queries, own_keys, own_values, cand_lengths = inputs
    head_group = QH // KVH
    score_scale = 1.0 / math.sqrt(HD)
    query_grid = group_queries.astype(jnp.float32).reshape(ROWS, KVH, head_group, HD)
    key_prefix = prefix_keys.astype(jnp.float32).reshape(PREFIX, KVH, HD)
    value_prefix = prefix_values.astype(jnp.float32).reshape(PREFIX, KVH, HD)
    prefix_scores = jnp.einsum('rkgd,pkd->kgrp', query_grid, key_prefix) * score_scale
    cand_queries = query_grid.reshape(CANDS, CLEN, KVH, head_group, HD)
    key_grid = own_keys.astype(jnp.float32).reshape(CANDS, CLEN, KVH, HD)
    value_grid = own_values.astype(jnp.float32).reshape(CANDS, CLEN, KVH, HD)
    own_scores = jnp.einsum('cikgd,cjkd->kgcij', cand_queries, key_grid) * score_scale
    live_mask = jnp.arange(CLEN, dtype=jnp.int32)[None, :] < cand_lengths[:, None]
    own_scores = jnp.where(live_mask[None, None, :, None, :], own_scores, NEG)
    row_max = jnp.maximum(lax.optimization_barrier(jnp.max(prefix_scores, -1)), lax.optimization_barrier(jnp.max(own_scores, -1)).reshape(KVH, head_group, ROWS))
    expo_prefix = jnp.exp(prefix_scores - row_max[..., None])
    expo_own = jnp.exp(own_scores - row_max.reshape(KVH, head_group, CANDS, CLEN)[..., None])
    row_total = lax.optimization_barrier(jnp.sum(expo_prefix, -1)) + lax.optimization_barrier(jnp.sum(expo_own, -1)).reshape(KVH, head_group, ROWS)
    weight_prefix = lax.optimization_barrier(expo_prefix.astype(jnp.bfloat16)).astype(jnp.float32)
    weight_own = lax.optimization_barrier(expo_own.astype(jnp.bfloat16)).astype(jnp.float32)
    weighted = jnp.einsum('kgrp,pkd->kgrd', weight_prefix, value_prefix)
    weighted = weighted + jnp.einsum('kgcij,cjkd->kgcid', weight_own, value_grid).reshape(KVH, head_group, ROWS, HD)
    context = weighted / row_total[..., None]
    context = jnp.transpose(context, (2, 0, 1, 3)).reshape(ROWS, QH * HD)
    return lax.optimization_barrier(context.astype(jnp.bfloat16))

def reference(queries, cand_keys, cand_values, prefix_kv, owner, lengths, out_weight):
    prefix = lax.dynamic_index_in_dim(prefix_kv, owner[0].astype(jnp.int32), 0, keepdims=False)
    weight_parts = out_weight.astype(jnp.float32).reshape(N_TP, QH * HD // N_TP, DWIN)

    def per_group(inputs):
        context = group_context(inputs, prefix[0], prefix[1])
        context_parts = context.astype(jnp.float32).reshape(ROWS, N_TP, QH * HD // N_TP)
        partial_value = jnp.einsum('rtc,tcd->trd', context_parts, weight_parts)
        rounded = lax.optimization_barrier(partial_value.astype(jnp.bfloat16)).astype(jnp.float32)
        return lax.optimization_barrier(jnp.sum(rounded, 0)).astype(jnp.bfloat16)
    grouped = lax.map(per_group, (queries.reshape(GROUPS, ROWS, QH * HD), cand_keys.reshape(GROUPS, ROWS, KVH * HD), cand_values.reshape(GROUPS, ROWS, KVH * HD), lengths))
    return grouped.reshape(GROUPS * ROWS, DWIN)
```

```python
import functools
import math

import jax
import jax.numpy as jnp
from jax import lax
from jax.experimental import pallas as pl
from jax.experimental.pallas import tpu as pltpu
from jax.sharding import PartitionSpec as P

HEADS = 8
HD = 128
CLEN = 128
PIECE = 256
NEG = -1e30
SCALE = math.log2(math.e) / math.sqrt(HD)
RB = 256


REP = [(y, z, c) for y in range(2) for z in range(8) for c in range(2)]
TP = [(y, x) for y in range(2) for x in range(4)]


def rep_id(y, z, c):
    return y * 16 + (z % 8) * 2 + c


def tp_id(y, x):
    return y * 4 + x % 4


CORE_SWAP = [(rep_id(*r), rep_id(r[0], r[1], 1 - r[2])) for r in REP]
YHI_SWAP = [(rep_id(*r), rep_id(1 - r[0], r[1], r[2])) for r in REP]
YLO_SWAP = [(tp_id(y, x), tp_id(1 - y, x)) for y, x in TP]


def z_shift(d):
    return [(rep_id(y, z, c), rep_id(y, z + d, c)) for y, z, c in REP]


def x_shift(d):
    return [(tp_id(y, x), tp_id(y, x + d)) for y, x in TP]


def lanes(s):
    return [s[:, i * 128 : (i + 1) * 128] for i in range(s.shape[1] // 128)]


def absorb(q, keys, values, masks, m_old, acc_old):
    cols = []
    for k, mask in zip(keys, masks):
        s = lanes(lax.dot_general(q, k, (((1,), (1,)), ((), ())), preferred_element_type=jnp.float32))
        if mask is not None:
            s = [jnp.where(ok, t, NEG) for ok, t in zip(mask, s)]
        cols += s
    top = jnp.max(functools.reduce(jnp.maximum, cols), axis=1, keepdims=True)
    m_new = jnp.broadcast_to(top, (q.shape[0], 128)) if m_old is None else jnp.maximum(m_old, top)
    shift = m_new * SCALE
    p = jnp.concatenate([jnp.exp2(t * SCALE - shift).astype(jnp.bfloat16) for t in cols], axis=1)
    v = jnp.concatenate(values, axis=0)
    v = jnp.concatenate([v, jnp.ones(v.shape, jnp.bfloat16)], axis=1)
    pv = jnp.dot(p, v, preferred_element_type=jnp.float32)
    if m_old is None:
        return m_new, pv
    decay = jnp.exp2(m_old * SCALE - shift)
    return m_new, acc_old * jnp.concatenate([decay, decay], axis=1) + pv


def pieces(refs):
    keys = [r[j, 0] for r in refs for j in range(r.shape[0])]
    values = [r[j, 1] for r in refs for j in range(r.shape[0])]
    return keys, values


def first_kernel(lens, q_ref, ck, cv, a0, m_out, acc_out):
    keys, values = pieces([a0])
    for i in range(q_ref.shape[0] // RB):
        r = pl.ds(i * RB, RB)
        slot = (lax.broadcasted_iota(jnp.int32, (RB, 128), 0) % 128) // 64
        lane = lax.broadcasted_iota(jnp.int32, (RB, 128), 1)
        mask = [(slot == t) & (lane < lens[t]) for t in range(2)]
        m, acc = absorb(q_ref[r], [ck[...]] + keys, [cv[...]] + values, [mask] + [None] * len(keys), None, None)
        m_out[r] = m
        acc_out[r] = acc


def mid_kernel(n, q_ref, *refs):
    keys, values = pieces(refs[:n])
    m_in, acc_in, m_out, acc_out = refs[n:]
    for i in range(q_ref.shape[0] // RB):
        r = pl.ds(i * RB, RB)
        m, acc = absorb(q_ref[r], keys, values, [None] * len(keys), m_in[r], acc_in[r])
        m_out[r] = m
        acc_out[r] = acc


W_PARTS = 4


def last_kernel(n, q_ref, *refs):
    kv = refs[:n]
    m_in, acc_in, w_hbm = refs[n : n + 3]
    own_a, x1, x2, x3, own_b, yb = refs[n + 3 : n + 9]
    ctx, w_buf, sem = refs[n + 9 :]
    depth = w_hbm.shape[0] // W_PARTS
    copies = [
        pltpu.make_async_copy(w_hbm.at[pl.ds(k * depth, depth)], w_buf.at[pl.ds(k * depth, depth)], sem.at[k])
        for k in range(W_PARTS)
    ]
    for c in copies:
        c.start()
    keys, values = pieces(kv)
    per = RB // 128
    for i in range(q_ref.shape[0] // RB):
        r = pl.ds(i * RB, RB)
        m, acc = absorb(q_ref[r], keys, values, [None] * len(keys), m_in[r], acc_in[r])
        out = (acc[:, :128] / acc[:, 128:]).astype(jnp.bfloat16)
        for j in range(per):
            ctx[:, pl.ds((i * per + j) * 128, 128)] = out[j * 128 : (j + 1) * 128]
    for c in copies:
        c.wait()
    block = 512
    half = own_a.shape[2]
    for c0 in range(0, 2 * half, block):
        y = jnp.dot(ctx[...], w_buf[:, pl.ds(c0, block)], preferred_element_type=jnp.float32).astype(jnp.bfloat16)
        if c0 < half:
            for dy in range(2):
                for dx, ref in enumerate((own_a, x1, x2, x3)):
                    ref[dy, :, pl.ds(c0, block)] = y[dy * 64 + dx * 16 : dy * 64 + dx * 16 + 16]
        else:
            for dy, ref in enumerate((own_b, yb)):
                for dx in range(4):
                    ref[dx, :, pl.ds(c0 - half, block)] = y[dy * 64 + dx * 16 : dy * 64 + dx * 16 + 16]


VM = pl.BlockSpec(memory_space=pltpu.VMEM)
SM = pl.BlockSpec(memory_space=pltpu.SMEM)
ANY = pl.BlockSpec(memory_space=pl.ANY)


def cost(rows, keys, extra=0):
    return pl.CostEstimate(flops=4 * rows * keys * HD + extra, transcendentals=rows * keys, bytes_accessed=0)


def state_shapes(rows):
    return (jax.ShapeDtypeStruct((rows, 128), jnp.float32), jax.ShapeDtypeStruct((rows, 256), jnp.float32))


def first_call(lens, q, ck, cv, a0):
    rows = q.shape[0]
    return pl.pallas_call(
        first_kernel,
        out_shape=state_shapes(rows),
        in_specs=[SM] + [VM] * 4,
        out_specs=(VM, VM),
        cost_estimate=cost(rows, 512),
        compiler_params=pltpu.CompilerParams(vmem_limit_bytes=20 << 20),
        name="attn_first",
    )(lens, q, ck, cv, a0)


def row_spec(width, index):
    return pl.BlockSpec((1024, width), lambda i: (index, 0))


def key_count(kvs):
    return sum(a.shape[0] for a in kvs) * PIECE


def full_spec(a):
    return pl.BlockSpec(a.shape, lambda i: (0,) * a.ndim)


def mid_call(q, kvs, state, chunk=None):
    n = len(kvs)
    rows = q.shape[0] if chunk is None else 1024
    index = 0 if chunk is None else chunk
    spec = lambda width: pl.BlockSpec((rows, width), lambda i: (index, 0))
    out_spec = lambda width: pl.BlockSpec((rows, width), lambda i: (0, 0))
    return pl.pallas_call(
        functools.partial(mid_kernel, n),
        grid=(1,),
        out_shape=state_shapes(rows),
        in_specs=[spec(128)] + [full_spec(a) for a in kvs] + [spec(128), spec(256)],
        out_specs=(out_spec(128), out_spec(256)),
        cost_estimate=cost(rows, key_count(kvs)),
        compiler_params=pltpu.CompilerParams(vmem_limit_bytes=24 << 20),
        name="attn_mid",
    )(q, *kvs, *state)


def last_call(q, kvs, state, w, chunk, state_chunk):
    n = len(kvs)
    spec = lambda width, index: pl.BlockSpec((1024, width), lambda i: (index, 0))
    half = w.shape[1] // 2
    tile = lambda k: jax.ShapeDtypeStruct((k, 16, half), jnp.bfloat16)
    outs = (tile(2), tile(2), tile(2), tile(2), tile(4), tile(4))
    return pl.pallas_call(
        functools.partial(last_kernel, n),
        grid=(1,),
        out_shape=outs,
        in_specs=[spec(128, chunk)]
        + [full_spec(a) for a in kvs]
        + [spec(128, state_chunk), spec(256, state_chunk), ANY],
        out_specs=tuple(full_spec(o) for o in outs),
        scratch_shapes=[
            pltpu.VMEM((128, w.shape[0]), jnp.bfloat16),
            pltpu.VMEM(w.shape, jnp.bfloat16),
            pltpu.SemaphoreType.DMA((W_PARTS,)),
        ],
        cost_estimate=cost(1024, key_count(kvs), 2 * 128 * w.shape[0] * w.shape[1]),
        compiler_params=pltpu.CompilerParams(vmem_limit_bytes=32 << 20),
        name="attn_last",
    )(q, *kvs, *state, w)


def f32(a):
    return a.astype(jnp.float32)


def reduce_rows(own_a, x1, x2, x3, own_b, yb):
    to_tp = functools.partial(lax.ppermute, axis_name="tp")
    r1 = to_tp(x1, perm=x_shift(1))
    r3 = to_tp(x3, perm=x_shift(-1))
    ry = to_tp(yb, perm=YLO_SWAP)
    r2 = to_tp(x2, perm=x_shift(2))
    s = f32(own_a) + f32(r1) + f32(r3) + f32(r2)
    u = f32(own_b) + f32(ry)
    ub = u.astype(jnp.bfloat16)
    t1 = to_tp(ub[1], perm=x_shift(1))
    t3 = to_tp(ub[3], perm=x_shift(-1))
    ty = to_tp(s[1].astype(jnp.bfloat16), perm=YLO_SWAP)
    t2 = to_tp(ub[2], perm=x_shift(2))
    left = s[0] + f32(ty)
    right = u[0] + f32(t1) + f32(t3) + f32(t2)
    return jnp.concatenate([left, right], axis=1).astype(jnp.bfloat16)


def body(queries, cand_keys, cand_values, prefix_kv, owner, lengths, out_weight):
    rep = lax.axis_index("rep")
    my_yh, my_z, my_c = rep // 16, (rep // 2) % 8, rep % 2
    tp = lax.axis_index("tp")
    my_yl, my_x = tp // 4, tp % 4
    root = owner[0]
    root_yh, root_z, root_c = root // 16, (root // 2) % 8, root % 2
    over_rep = functools.partial(lax.ppermute, axis_name="rep")

    q = queries.reshape(2, 4, 2, 16, HEADS, HD)
    q = jnp.where(my_yl == 0, q, q[::-1])
    q = lax.dynamic_slice_in_dim(jnp.concatenate([q, q], axis=1), my_x, 4, 1)
    q = jnp.transpose(q, (2, 4, 0, 1, 3, 5)).reshape(2048, HD)
    flip = lambda a: jnp.where(my_yl == 0, a, a[::-1])
    ck = flip(cand_keys.reshape(2, CLEN, HD)).reshape(2 * CLEN, HD)
    cv = flip(cand_values.reshape(2, CLEN, HD)).reshape(2 * CLEN, HD)
    lens = flip(lengths[0])

    prefix = prefix_kv[0]
    half_keys = prefix.shape[1] // 2
    half_of = lambda c: lax.dynamic_slice_in_dim(prefix, c * half_keys, half_keys, 1)
    from_partner = over_rep(half_of(1 - my_c), perm=CORE_SWAP)
    half = jnp.where(my_c == root_c, half_of(my_c), from_partner)
    piece = lambda d: lax.dynamic_slice_in_dim(half, ((my_z + d) % 8) * PIECE, PIECE, 1)
    outgoing = [piece(d) for d in range(1, 8)]

    def branch(b):
        def send(*parts):
            got = []
            for d in (4, 3, 5, 2, 6, 1, 7):
                apart = {1: 1, 2: 2, 3: 4, 4: 4}[min(d, 8 - d)]
                roots = [z for z in range(8) if z % apart == b % apart]
                pairs = [(rep_id(y, z, c), rep_id(y, z + d, c)) for y in range(2) for z in roots for c in range(2)]
                got.append((d, over_rep(parts[d - 1], perm=pairs)))
            return tuple(v for _, v in sorted(got))

        return send

    got = lax.switch(root_z % 4, [branch(b) for b in range(4)], *outgoing)
    away = (my_z - root_z) % 8
    mine = lax.select_n(away, piece(0), *got)
    across = over_rep(mine, perm=YHI_SWAP)
    a0 = jnp.where(my_yh == root_yh, mine, across)[None]

    above = over_rep(a0, perm=z_shift(-1))
    below = over_rep(a0, perm=z_shift(1))
    facing = over_rep(a0, perm=z_shift(4))
    c0 = over_rep(a0, perm=CORE_SWAP)
    state = first_call(lens, q, ck, cv, a0)
    above, below, facing, c0, state = lax.optimization_barrier((above, below, facing, c0, state))

    far_above = over_rep(jnp.concatenate([above, facing]), perm=z_shift(-1))
    far_below = over_rep(jnp.concatenate([below, facing]), perm=z_shift(1))
    c1 = over_rep(jnp.concatenate([above, below, facing]), perm=CORE_SWAP)
    state = mid_call(q, [above, below, facing, c0], state)
    far_above, far_below, c1, state = lax.optimization_barrier((far_above, far_below, c1, state))

    c2 = over_rep(jnp.concatenate([far_above, far_below]), perm=CORE_SWAP)
    late = [far_above, far_below, c1]
    state_0 = mid_call(q, late, state, 0)
    tiles_0 = last_call(q, [c2], state_0, out_weight, 0, 0)
    tiles_1 = last_call(q, late + [c2], state, out_weight, 1, 1)
    out_0 = reduce_rows(*tiles_0)
    out_1 = reduce_rows(*tiles_1)
    return jnp.concatenate([out_0, out_1], axis=0)


def solution(mesh):
    in_specs = (
        P("rep", "tp"),
        P("rep", "tp"),
        P("rep", "tp"),
        P("rep", None, None, "tp"),
        P(),
        P("rep", None),
        P("tp", None),
    )
    out_specs = P(("rep", "tp"), None)
    return jax.shard_map(body, mesh=mesh, in_specs=in_specs, out_specs=out_specs, check_vma=False)
```

```python
import functools
import math

import jax
import jax.numpy as jnp
from jax import lax
from jax.experimental import pallas as pl
from jax.experimental.pallas import tpu as pltpu
from jax.sharding import PartitionSpec as P

HEADS = 8
HD = 128
CLEN = 128
PIECE = 256
NEG = -1e30
SCALE = math.log2(math.e) / math.sqrt(HD)


REP = [(y, z, c) for y in range(2) for z in range(8) for c in range(2)]
TP = [(y, x) for y in range(2) for x in range(4)]


def rep_id(y, z, c):
    return y * 16 + (z % 8) * 2 + c


def tp_id(y, x):
    return y * 4 + x % 4


CORE_SWAP = [(rep_id(*r), rep_id(r[0], r[1], 1 - r[2])) for r in REP]
YHI_SWAP = [(rep_id(*r), rep_id(1 - r[0], r[1], r[2])) for r in REP]
YLO_SWAP = [(tp_id(y, x), tp_id(1 - y, x)) for y, x in TP]


def z_shift(d):
    return [(rep_id(y, z, c), rep_id(y, z + d, c)) for y, z, c in REP]


def x_shift(d):
    return [(tp_id(y, x), tp_id(y, x + d)) for y, x in TP]


def lanes(s):
    return [s[:, i * 128 : (i + 1) * 128] for i in range(s.shape[1] // 128)]


def absorb(q, keys, values, masks, m_old, acc_old):
    cols = []
    for k, mask in zip(keys, masks):
        s = lanes(lax.dot_general(q, k, (((1,), (1,)), ((), ())), preferred_element_type=jnp.float32))
        if mask is not None:
            s = [jnp.where(ok, t, NEG) for ok, t in zip(mask, s)]
        cols += s
    top = jnp.max(functools.reduce(jnp.maximum, cols), axis=1, keepdims=True)
    m_new = jnp.broadcast_to(top, (q.shape[0], 128)) if m_old is None else jnp.maximum(m_old, top)
    shift = m_new * SCALE
    p = jnp.concatenate([jnp.exp2(t * SCALE - shift).astype(jnp.bfloat16) for t in cols], axis=1)
    v = jnp.concatenate(values, axis=0)
    v = jnp.concatenate([v, jnp.ones(v.shape, jnp.bfloat16)], axis=1)
    pv = jnp.dot(p, v, preferred_element_type=jnp.float32)
    if m_old is None:
        return m_new, pv
    decay = jnp.exp2(m_old * SCALE - shift)
    return m_new, acc_old * jnp.concatenate([decay, decay], axis=1) + pv


def pieces(refs):
    keys = [r[j, 0] for r in refs for j in range(r.shape[0])]
    values = [r[j, 1] for r in refs for j in range(r.shape[0])]
    return keys, values


UNROLL = 8


def each_head(f):
    def step(i, carry):
        for j in range(UNROLL):
            f(i * UNROLL + j)
        return carry

    lax.fori_loop(0, HEADS // UNROLL, step, 0)


def head_cols(h):
    return pl.ds(pl.multiple_of(h * HD, HD), HD)


def first_kernel(lens, q_ref, ck, cv, a0, m_out, acc_out):
    rows = q_ref.shape[0]

    def head(h):
        keys, values = pieces([a0])
        slot = lax.broadcasted_iota(jnp.int32, (rows, 128), 0) // CLEN
        lane = lax.broadcasted_iota(jnp.int32, (rows, 128), 1)
        mask = [(slot == t) & (lane < lens[t]) for t in range(2)]
        q = q_ref[:, head_cols(h)]
        m_out[h], acc_out[h] = absorb(
            q, [ck[...]] + keys, [cv[...]] + values, [mask] + [None] * len(keys), None, None
        )

    each_head(head)


def mid_kernel(n, q_ref, *refs):
    m_in, acc_in, m_out, acc_out = refs[n:]

    def head(h):
        keys, values = pieces(refs[:n])
        q = q_ref[:, head_cols(h)]
        m_out[h], acc_out[h] = absorb(q, keys, values, [None] * len(keys), m_in[h], acc_in[h])

    each_head(head)


W_BLOCK = 512


def last_kernel(n, spot, q_ref, *refs):
    m_in, acc_in, w, own_a, x1, x2, x3, own_b, yb, ctx = refs[n:]

    def head(h):
        keys, values = pieces(refs[:n])
        q = q_ref[:, head_cols(h)]
        _, acc = absorb(q, keys, values, [None] * len(keys), m_in[h], acc_in[h])
        ctx[:, head_cols(h)] = (acc[:, :HD] / acc[:, HD:]).astype(jnp.bfloat16)

    each_head(head)

    tile = own_a.shape[1]
    half = own_a.shape[2]
    tp_of = [((spot[0] + dy) % 2) * 4 + (spot[1] + dx) % 4 for dy in range(2) for dx in range(4)]
    rel = jnp.concatenate([ctx[pl.ds(pl.multiple_of(t * tile, tile), tile)] for t in tp_of], axis=0)

    def product(c):
        return jnp.dot(rel, w[:, pl.ds(c, W_BLOCK)], preferred_element_type=jnp.float32).astype(jnp.bfloat16)

    for c in range(0, half, W_BLOCK):
        y = product(half + c)
        for dy, ref in enumerate((own_b, yb)):
            for dx in range(4):
                ref[dx, :, pl.ds(c, W_BLOCK)] = y[(dy * 4 + dx) * tile : (dy * 4 + dx + 1) * tile]
        y = product(c)
        for dx, ref in enumerate((own_a, x1, x2, x3)):
            for dy in range(2):
                ref[dy, :, pl.ds(c, W_BLOCK)] = y[(dy * 4 + dx) * tile : (dy * 4 + dx + 1) * tile]


VM = pl.BlockSpec(memory_space=pltpu.VMEM)
SM = pl.BlockSpec(memory_space=pltpu.SMEM)


def cost(rows, keys, extra=0):
    return pl.CostEstimate(
        flops=4 * rows * HEADS * keys * HD + extra, transcendentals=rows * HEADS * keys, bytes_accessed=0
    )


def state_shapes(rows):
    return (
        jax.ShapeDtypeStruct((HEADS, rows, HD), jnp.float32),
        jax.ShapeDtypeStruct((HEADS, rows, 2 * HD), jnp.float32),
    )


def key_count(kvs):
    return sum(a.shape[0] for a in kvs) * PIECE


def first_call(lens, q, ck, cv, a0):
    rows = q.shape[0]
    return pl.pallas_call(
        first_kernel,
        out_shape=state_shapes(rows),
        in_specs=[SM] + [VM] * 4,
        out_specs=(VM, VM),
        cost_estimate=cost(rows, 2 * PIECE),
        compiler_params=pltpu.CompilerParams(vmem_limit_bytes=12 << 20),
        name="attn_first",
    )(lens, q, ck, cv, a0)


def mid_call(q, kvs, state):
    n = len(kvs)
    rows = q.shape[0]
    return pl.pallas_call(
        functools.partial(mid_kernel, n),
        out_shape=state_shapes(rows),
        in_specs=[VM] * (n + 3),
        out_specs=(VM, VM),
        input_output_aliases={n + 1: 0, n + 2: 1},
        cost_estimate=cost(rows, key_count(kvs)),
        compiler_params=pltpu.CompilerParams(vmem_limit_bytes=12 << 20),
        name="attn_mid",
    )(q, *kvs, *state)


def last_call(spot, q, kvs, state, w):
    n = len(kvs)
    rows = q.shape[0]
    part = lambda k: jax.ShapeDtypeStruct((k, rows // 8, w.shape[1] // 2), jnp.bfloat16)
    outs = (part(2), part(2), part(2), part(2), part(4), part(4))
    return pl.pallas_call(
        functools.partial(last_kernel, n),
        out_shape=outs,
        in_specs=[SM] + [VM] * (n + 4),
        out_specs=(VM,) * len(outs),
        scratch_shapes=[pltpu.VMEM((rows, w.shape[0]), jnp.bfloat16)],
        cost_estimate=cost(rows, key_count(kvs), 2 * rows * w.shape[0] * w.shape[1]),
        compiler_params=pltpu.CompilerParams(vmem_limit_bytes=12 << 20),
        name="attn_last",
    )(spot, q, *kvs, *state, w)


def f32(a):
    return a.astype(jnp.float32)


def reduce_rows(own_a, x1, x2, x3, own_b, yb):
    over_tp = functools.partial(lax.ppermute, axis_name="tp")
    ry = over_tp(yb, perm=YLO_SWAP)
    r2 = over_tp(x2, perm=x_shift(2))
    r1 = over_tp(x1, perm=x_shift(1))
    r3 = over_tp(x3, perm=x_shift(-1))
    s = f32(own_a) + f32(r1) + f32(r3) + f32(r2)
    u = f32(own_b) + f32(ry)
    ub = u.astype(jnp.bfloat16)
    t2 = over_tp(ub[2], perm=x_shift(2))
    t1 = over_tp(ub[1], perm=x_shift(1))
    t3 = over_tp(ub[3], perm=x_shift(-1))
    ty = over_tp(s[1].astype(jnp.bfloat16), perm=YLO_SWAP)
    left = s[0] + f32(ty)
    right = u[0] + f32(t1) + f32(t3) + f32(t2)
    return jnp.concatenate([left, right], axis=1).astype(jnp.bfloat16)


def body(queries, cand_keys, cand_values, prefix_kv, owner, lengths, out_weight):
    rep = lax.axis_index("rep")
    my_yh, my_z, my_c = rep // 16, (rep // 2) % 8, rep % 2
    tp = lax.axis_index("tp")
    spot = jnp.stack([tp // 4, tp % 4]).astype(jnp.int32)
    root = owner[0]
    root_yh, root_z, root_c = root // 16, (root // 2) % 8, root % 2
    over_rep = functools.partial(lax.ppermute, axis_name="rep")

    prefix = prefix_kv[0]
    partner = over_rep(prefix, perm=CORE_SWAP)
    mine = my_c == root_c
    up = 1 - 2 * my_c
    pick = lambda start, size: jnp.where(
        mine,
        lax.dynamic_slice_in_dim(prefix, start, size, 1),
        lax.dynamic_slice_in_dim(partner, start, size, 1),
    )
    whole = lambda d: pick(((my_z + up * d) % 8) * 2 * PIECE, 2 * PIECE)
    opposite = pick(((my_z + 4) % 8) * 2 * PIECE + my_c * PIECE, PIECE)
    steps = (my_z - root_z) % 8
    steps = jnp.where(my_c == 0, steps, (8 - steps) % 8)

    def branch(b):
        def send(steps, own, *parts):
            got = {}
            for d in (3, 4, 2, 1):
                pairs = [
                    (rep_id(y, z, c), rep_id(y, z + (1 - 2 * c) * d, c))
                    for y in range(2)
                    for z in (b, b + 4)
                    for c in range(2)
                ]
                got[d] = over_rep(parts[d - 1], perm=pairs)
            got[4] = jnp.concatenate([got[4], got[4]], axis=1)
            return lax.select_n(jnp.minimum(steps, 4), own, got[1], got[2], got[3], got[4])

        return send

    slot = lax.switch(
        root_z % 4, [branch(b) for b in range(4)], steps, whole(0), whole(1), whole(2), whole(3), opposite
    )
    half_of = lambda a, c: lax.dynamic_slice_in_dim(a, c * PIECE, PIECE, 1)
    from_partner = over_rep(half_of(slot, 1 - my_c), perm=CORE_SWAP)
    piece = jnp.where(steps <= 4, half_of(slot, my_c), from_partner)
    across = over_rep(piece, perm=YHI_SWAP)
    a0 = jnp.where(my_yh == root_yh, piece, across)[None]
    a0, spot = lax.optimization_barrier((a0, spot))

    above = over_rep(a0, perm=z_shift(-1))
    below = over_rep(a0, perm=z_shift(1))
    facing = over_rep(a0, perm=z_shift(4))
    state = first_call(lengths[0], queries, cand_keys, cand_values, a0)
    above, below, facing, state = lax.optimization_barrier((above, below, facing, state))

    far_above = over_rep(jnp.concatenate([above, facing]), perm=z_shift(-1))
    far_below = over_rep(jnp.concatenate([below, facing]), perm=z_shift(1))
    near_other = over_rep(jnp.concatenate([a0, above, below, facing]), perm=CORE_SWAP)
    state = mid_call(queries, [above, below, facing], state)
    state = mid_call(queries, [near_other], state)
    far_above, far_below, state = lax.optimization_barrier((far_above, far_below, state))

    far_other = over_rep(jnp.concatenate([far_above, far_below]), perm=CORE_SWAP)
    state = mid_call(queries, [far_above, far_below], state)
    return reduce_rows(*last_call(spot, queries, [far_other], state, out_weight))


def solution(mesh):
    in_specs = (
        P("rep", "tp"),
        P("rep", "tp"),
        P("rep", "tp"),
        P("rep", None, None, "tp"),
        P(),
        P("rep", None),
        P("tp", None),
    )
    out_specs = P(("rep", "tp"), None)
    return jax.shard_map(body, mesh=mesh, in_specs=in_specs, out_specs=out_specs, check_vma=False)
```

```python
import functools
import math

import jax
import jax.numpy as jnp
from jax import lax
from jax.experimental import pallas as pl
from jax.experimental.pallas import tpu as pltpu
from jax.sharding import PartitionSpec as P

HEADS = 8
HD = 128
CLEN = 128
PIECE = 256
NEG = -1e30
SCALE = math.log2(math.e) / math.sqrt(HD)


REP = [(y, z, c) for y in range(2) for z in range(8) for c in range(2)]
TP = [(y, x) for y in range(2) for x in range(4)]


def rep_id(y, z, c):
    return y * 16 + (z % 8) * 2 + c


def tp_id(y, x):
    return y * 4 + x % 4


CORE_SWAP = [(rep_id(*r), rep_id(r[0], r[1], 1 - r[2])) for r in REP]
YHI_SWAP = [(rep_id(*r), rep_id(1 - r[0], r[1], r[2])) for r in REP]
YLO_SWAP = [(tp_id(y, x), tp_id(1 - y, x)) for y, x in TP]


def z_shift(d):
    return [(rep_id(y, z, c), rep_id(y, z + d, c)) for y, z, c in REP]


def x_shift(d):
    return [(tp_id(y, x), tp_id(y, x + d)) for y, x in TP]


def lanes(s):
    return [s[:, i * 128 : (i + 1) * 128] for i in range(s.shape[1] // 128)]


def absorb(q, keys, values, masks, m_old, acc_old):
    cols = []
    for k, mask in zip(keys, masks):
        s = lanes(lax.dot_general(q, k, (((1,), (1,)), ((), ())), preferred_element_type=jnp.float32))
        if mask is not None:
            s = [jnp.where(ok, t, NEG) for ok, t in zip(mask, s)]
        cols += s
    top = jnp.max(functools.reduce(jnp.maximum, cols), axis=1, keepdims=True)
    m_new = jnp.broadcast_to(top, (q.shape[0], 128)) if m_old is None else jnp.maximum(m_old, top)
    shift = m_new * SCALE
    p = jnp.concatenate([jnp.exp2(t * SCALE - shift).astype(jnp.bfloat16) for t in cols], axis=1)
    v = jnp.concatenate(values, axis=0)
    v = jnp.concatenate([v, jnp.ones(v.shape, jnp.bfloat16)], axis=1)
    pv = jnp.dot(p, v, preferred_element_type=jnp.float32)
    if m_old is None:
        return m_new, pv
    decay = jnp.exp2(m_old * SCALE - shift)
    return m_new, acc_old * jnp.concatenate([decay, decay], axis=1) + pv


def pieces(refs):
    keys = [r[j, 0] for r in refs for j in range(r.shape[0])]
    values = [r[j, 1] for r in refs for j in range(r.shape[0])]
    return keys, values


UNROLL = 8


def each_head(f, unroll=UNROLL):
    def step(i, carry):
        for j in range(unroll):
            f(i * unroll + j)
        return carry

    lax.fori_loop(0, HEADS // unroll, step, 0)


def head_cols(h):
    return pl.ds(pl.multiple_of(h * HD, HD), HD)


def first_kernel(lens, q_ref, ck, cv, a0, m_out, acc_out):
    rows = q_ref.shape[0]

    def head(h):
        keys, values = pieces([a0])
        slot = lax.broadcasted_iota(jnp.int32, (rows, 128), 0) // CLEN
        lane = lax.broadcasted_iota(jnp.int32, (rows, 128), 1)
        mask = [(slot == t) & (lane < lens[t]) for t in range(2)]
        q = q_ref[:, head_cols(h)]
        m_out[h], acc_out[h] = absorb(
            q, [ck[...]] + keys, [cv[...]] + values, [mask] + [None] * len(keys), None, None
        )

    each_head(head, 4)


def mid_kernel(n, q_ref, *refs):
    m_in, acc_in, m_out, acc_out = refs[n:]

    def head(h):
        keys, values = pieces(refs[:n])
        q = q_ref[:, head_cols(h)]
        m_out[h], acc_out[h] = absorb(q, keys, values, [None] * len(keys), m_in[h], acc_in[h])

    each_head(head)


W_BLOCK = 512


def product(rel, w, c):
    return jnp.dot(rel, w[:, pl.ds(c, W_BLOCK)], preferred_element_type=jnp.float32).astype(jnp.bfloat16)


def last_kernel(n, spot, q_ref, *refs):
    m_in, acc_in, w, rel_out, own_b, yb, ctx = refs[n:]

    def head(h):
        keys, values = pieces(refs[:n])
        q = q_ref[:, head_cols(h)]
        _, acc = absorb(q, keys, values, [None] * len(keys), m_in[h], acc_in[h])
        ctx[:, head_cols(h)] = (acc[:, :HD] / acc[:, HD:]).astype(jnp.bfloat16)

    each_head(head, 4)

    tile = own_b.shape[1]
    half = own_b.shape[2]
    tp_of = [((spot[0] + dy) % 2) * 4 + (spot[1] + dx) % 4 for dy in range(2) for dx in range(4)]
    rel = jnp.concatenate([ctx[pl.ds(pl.multiple_of(t * tile, tile), tile)] for t in tp_of], axis=0)
    rel_out[...] = rel
    for c in range(0, half, W_BLOCK):
        y = product(rel, w, half + c)
        for dy, ref in enumerate((own_b, yb)):
            for dx in range(4):
                ref[dx, :, pl.ds(c, W_BLOCK)] = y[(dy * 4 + dx) * tile : (dy * 4 + dx + 1) * tile]


def left_kernel(rel_ref, w, own_a, x1, x2, x3):
    tile = own_a.shape[1]
    rel = rel_ref[...]
    for c in range(0, own_a.shape[2], W_BLOCK):
        y = product(rel, w, c)
        for dx, ref in enumerate((own_a, x1, x2, x3)):
            for dy in range(2):
                ref[dy, :, pl.ds(c, W_BLOCK)] = y[(dy * 4 + dx) * tile : (dy * 4 + dx + 1) * tile]


VM = pl.BlockSpec(memory_space=pltpu.VMEM)
ANY = pl.BlockSpec(memory_space=pl.ANY)
SM = pl.BlockSpec(memory_space=pltpu.SMEM)


def cost(rows, keys, extra=0):
    return pl.CostEstimate(
        flops=4 * rows * HEADS * keys * HD + extra, transcendentals=rows * HEADS * keys, bytes_accessed=0
    )


def state_shapes(rows):
    return (
        jax.ShapeDtypeStruct((HEADS, rows, HD), jnp.float32),
        jax.ShapeDtypeStruct((HEADS, rows, 2 * HD), jnp.float32),
    )


def key_count(kvs):
    return sum(a.shape[0] for a in kvs) * PIECE


def moves(pairs, sem):
    copies = [pltpu.make_async_copy(source, target, sem.at[i]) for i, (source, target) in enumerate(pairs)]
    for copy in copies:
        copy.start()
    for copy in copies:
        copy.wait()


def windows(at, source):
    z, c = at[1], at[2]
    up = 1 - 2 * c
    spots = [(lax.rem(z + up * d + 8, 8) * 2 * PIECE, 2 * PIECE) for d in range(4)]
    spots.append((lax.rem(z + 4, 8) * 2 * PIECE + c * PIECE, PIECE))
    return [source.at[:, pl.ds(pl.multiple_of(start, PIECE), size)] for start, size in spots]


def cut_kernel(at, prefix, *refs):
    moves(zip(windows(at, prefix), refs[:-1]), refs[-1])


def choose_kernel(at, partner, *refs):
    mine, outs, sem = refs[:5], refs[5:10], refs[10]

    @pl.when(at[0] == 1)
    def _():
        moves(zip(mine, outs), sem)

    @pl.when(at[0] == 0)
    def _():
        moves(zip(windows(at, partner), outs), sem)


def cut_call(kernel, at, source, *mine):
    part = lambda size: jax.ShapeDtypeStruct((2, size, HD), jnp.bfloat16)
    return pl.pallas_call(
        kernel,
        out_shape=(part(2 * PIECE),) * 4 + (part(PIECE),),
        in_specs=[SM] + [ANY] * (1 + len(mine)),
        out_specs=(VM,) * 5,
        scratch_shapes=[pltpu.SemaphoreType.DMA((5,))],
        compiler_params=pltpu.CompilerParams(vmem_limit_bytes=4 << 20),
        cost_estimate=pl.CostEstimate(flops=1 << 28, transcendentals=0, bytes_accessed=0),
    )(at, source, *mine)


def first_call(lens, q, ck, cv, a0):
    rows = q.shape[0]
    return pl.pallas_call(
        first_kernel,
        out_shape=state_shapes(rows),
        in_specs=[SM] + [VM] * 4,
        out_specs=(VM, VM),
        cost_estimate=cost(rows, 2 * PIECE),
        compiler_params=pltpu.CompilerParams(vmem_limit_bytes=12 << 20),
        name="attn_first",
    )(lens, q, ck, cv, a0)


def mid_call(q, kvs, state):
    n = len(kvs)
    rows = q.shape[0]
    return pl.pallas_call(
        functools.partial(mid_kernel, n),
        out_shape=state_shapes(rows),
        in_specs=[VM] * (n + 3),
        out_specs=(VM, VM),
        input_output_aliases={n + 1: 0, n + 2: 1},
        cost_estimate=cost(rows, key_count(kvs)),
        compiler_params=pltpu.CompilerParams(vmem_limit_bytes=12 << 20),
        name="attn_mid",
    )(q, *kvs, *state)


def last_call(spot, q, kvs, state, w):
    n = len(kvs)
    rows = q.shape[0]
    part = lambda k: jax.ShapeDtypeStruct((k, rows // 8, w.shape[1] // 2), jnp.bfloat16)
    outs = (jax.ShapeDtypeStruct((rows, w.shape[0]), jnp.bfloat16), part(4), part(4))
    return pl.pallas_call(
        functools.partial(last_kernel, n),
        out_shape=outs,
        in_specs=[SM] + [VM] * (n + 4),
        out_specs=(VM,) * len(outs),
        scratch_shapes=[pltpu.VMEM((rows, w.shape[0]), jnp.bfloat16)],
        cost_estimate=cost(rows, key_count(kvs), rows * w.shape[0] * w.shape[1]),
        compiler_params=pltpu.CompilerParams(vmem_limit_bytes=12 << 20),
        name="attn_last",
    )(spot, q, *kvs, *state, w)


def left_call(rel, w):
    rows = rel.shape[0]
    part = jax.ShapeDtypeStruct((2, rows // 8, w.shape[1] // 2), jnp.bfloat16)
    return pl.pallas_call(
        left_kernel,
        out_shape=(part,) * 4,
        in_specs=[VM] * 2,
        out_specs=(VM,) * 4,
        cost_estimate=pl.CostEstimate(flops=rows * w.shape[0] * w.shape[1], transcendentals=0, bytes_accessed=0),
        compiler_params=pltpu.CompilerParams(vmem_limit_bytes=12 << 20),
        name="project_left",
    )(rel, w)


def f32(a):
    return a.astype(jnp.float32)


def reduce_rows(rel, own_b, yb, w):
    over_tp = functools.partial(lax.ppermute, axis_name="tp")
    ry = over_tp(yb, perm=YLO_SWAP)
    own_a, x1, x2, x3 = left_call(rel, w)
    r2 = over_tp(x2, perm=x_shift(2))
    r1 = over_tp(x1, perm=x_shift(1))
    r3 = over_tp(x3, perm=x_shift(-1))
    u = f32(own_b) + f32(ry)
    ub = u.astype(jnp.bfloat16)
    t1 = over_tp(ub[1], perm=x_shift(1))
    t3 = over_tp(ub[3], perm=x_shift(-1))
    t2 = over_tp(ub[2], perm=x_shift(2))
    s = f32(own_a) + f32(r1) + f32(r3) + f32(r2)
    ty = over_tp(s[1].astype(jnp.bfloat16), perm=YLO_SWAP)
    left = s[0] + f32(ty)
    right = u[0] + f32(t1) + f32(t3) + f32(t2)
    return jnp.concatenate([left, right], axis=1).astype(jnp.bfloat16)


def body(queries, cand_keys, cand_values, prefix_kv, owner, lengths, out_weight):
    rep = lax.axis_index("rep")
    my_yh, my_z, my_c = rep // 16, (rep // 2) % 8, rep % 2
    tp = lax.axis_index("tp")
    spot = jnp.stack([tp // 4, tp % 4]).astype(jnp.int32)
    root = owner[0]
    root_yh, root_z, root_c = root // 16, (root // 2) % 8, root % 2
    over_rep = functools.partial(lax.ppermute, axis_name="rep")

    cut_at = jnp.stack([my_c == root_c, my_z, my_c]).astype(jnp.int32)
    steps = (my_z - root_z) % 8
    steps = jnp.where(my_c == 0, steps, (8 - steps) % 8)
    prefix, cut_at, spot, steps, root_z, root_yh, my_c, my_yh = lax.optimization_barrier(
        (prefix_kv[0], cut_at, spot, steps, root_z, root_yh, my_c, my_yh)
    )
    partner = over_rep(prefix, perm=CORE_SWAP)
    parts = cut_call(cut_kernel, cut_at, prefix)
    own, *outgoing = cut_call(choose_kernel, cut_at, partner, *parts)

    def branch(b):
        def send(steps, own, *parts):
            got = {}
            for d in (3, 4, 2, 1):
                roots = {1: range(b % 2, 8, 2), 2: (b % 4, b % 4 + 4)}.get(d, (b,))
                pairs = [
                    (rep_id(y, z, c), rep_id(y, z + (1 - 2 * c) * d, c))
                    for y in range(2)
                    for z in roots
                    for c in range(2)
                ]
                got[d] = over_rep(parts[d - 1], perm=pairs)
            got[4] = jnp.concatenate([got[4], got[4]], axis=1)
            return lax.select_n(jnp.minimum(steps, 4), own, got[1], got[2], got[3], got[4])

        return send

    slot = lax.switch(root_z, [branch(b) for b in range(8)], steps, own, *outgoing)
    half_of = lambda a, c: lax.dynamic_slice_in_dim(a, c * PIECE, PIECE, 1)
    from_partner = over_rep(half_of(slot, 1 - my_c), perm=CORE_SWAP)
    piece = jnp.where(steps <= 4, half_of(slot, my_c), from_partner)
    across = over_rep(piece, perm=YHI_SWAP)
    a0 = jnp.where(my_yh == root_yh, piece, across)[None]

    facing = over_rep(a0, perm=z_shift(4))
    above = over_rep(a0, perm=z_shift(-1))
    below = over_rep(a0, perm=z_shift(1))
    state = first_call(lengths[0], queries, cand_keys, cand_values, a0)
    above, below, facing, state = lax.optimization_barrier((above, below, facing, state))

    far_above = over_rep(jnp.concatenate([above, facing]), perm=z_shift(-1))
    far_below = over_rep(jnp.concatenate([below, facing]), perm=z_shift(1))
    near_other = over_rep(jnp.concatenate([a0, above, below, facing]), perm=CORE_SWAP)
    state = mid_call(queries, [above, below, facing], state)
    state = mid_call(queries, [near_other], state)
    far_above, far_below, state = lax.optimization_barrier((far_above, far_below, state))

    far_other = over_rep(jnp.concatenate([far_above, far_below]), perm=CORE_SWAP)
    state = mid_call(queries, [far_above, far_below], state)
    return reduce_rows(*last_call(spot, queries, [far_other], state, out_weight), out_weight)


def solution(mesh):
    in_specs = (
        P("rep", "tp"),
        P("rep", "tp"),
        P("rep", "tp"),
        P("rep", None, None, "tp"),
        P(),
        P("rep", None),
        P("tp", None),
    )
    out_specs = P(("rep", "tp"), None)
    return jax.shard_map(body, mesh=mesh, in_specs=in_specs, out_specs=out_specs, check_vma=False)
```

```python
import functools
import math

import jax
import jax.numpy as jnp
from jax import lax
from jax.experimental import pallas as pl
from jax.experimental.pallas import tpu as pltpu
from jax.sharding import PartitionSpec as P

HEADS = 8
HD = 128
CLEN = 128
PIECE = 256
NEG = -1e30
SCALE = math.log2(math.e) / math.sqrt(HD)


REP = [(y, z, c) for y in range(2) for z in range(8) for c in range(2)]
TP = [(y, x) for y in range(2) for x in range(4)]


def rep_id(y, z, c):
    return y * 16 + (z % 8) * 2 + c


def tp_id(y, x):
    return y * 4 + x % 4


CORE_SWAP = [(rep_id(*r), rep_id(r[0], r[1], 1 - r[2])) for r in REP]
YHI_SWAP = [(rep_id(*r), rep_id(1 - r[0], r[1], r[2])) for r in REP]
YLO_SWAP = [(tp_id(y, x), tp_id(1 - y, x)) for y, x in TP]


def z_shift(d):
    return [(rep_id(y, z, c), rep_id(y, z + d, c)) for y, z, c in REP]


def x_shift(d):
    return [(tp_id(y, x), tp_id(y, x + d)) for y, x in TP]


def lanes(s):
    return [s[:, i * 128 : (i + 1) * 128] for i in range(s.shape[1] // 128)]


def absorb(q, keys, values, masks, m_old, acc_old):
    cols = []
    for k, mask in zip(keys, masks):
        s = lanes(lax.dot_general(q, k, (((1,), (1,)), ((), ())), preferred_element_type=jnp.float32))
        if mask is not None:
            s = [jnp.where(ok, t, NEG) for ok, t in zip(mask, s)]
        cols += s
    top = jnp.max(functools.reduce(jnp.maximum, cols), axis=1, keepdims=True)
    m_new = jnp.broadcast_to(top, (q.shape[0], 128)) if m_old is None else jnp.maximum(m_old, top)
    shift = m_new * SCALE
    p = jnp.concatenate([jnp.exp2(t * SCALE - shift).astype(jnp.bfloat16) for t in cols], axis=1)
    v = jnp.concatenate(values, axis=0)
    v = jnp.concatenate([v, jnp.ones(v.shape, jnp.bfloat16)], axis=1)
    pv = jnp.dot(p, v, preferred_element_type=jnp.float32)
    if m_old is None:
        return m_new, pv
    decay = jnp.exp2(m_old * SCALE - shift)
    return m_new, acc_old * jnp.concatenate([decay, decay], axis=1) + pv


def pieces(refs):
    keys = [r[j, 0] for r in refs for j in range(r.shape[0])]
    values = [r[j, 1] for r in refs for j in range(r.shape[0])]
    return keys, values


UNROLL = 8


def each_head(f, unroll=UNROLL):
    def step(i, carry):
        for j in range(unroll):
            f(i * unroll + j)
        return carry

    lax.fori_loop(0, HEADS // unroll, step, 0)


def head_cols(h):
    return pl.ds(pl.multiple_of(h * HD, HD), HD)


def first_kernel(lens, q_ref, ck, cv, *refs):
    m_out, acc_out = refs[-2:]
    rows = q_ref.shape[0]

    def head(h):
        keys, values = pieces(refs[:-2])
        slot = lax.broadcasted_iota(jnp.int32, (rows, 128), 0) // CLEN
        lane = lax.broadcasted_iota(jnp.int32, (rows, 128), 1)
        mask = [(slot == t) & (lane < lens[t]) for t in range(2)]
        q = q_ref[:, head_cols(h)]
        m_out[h], acc_out[h] = absorb(
            q, [ck[...]] + keys, [cv[...]] + values, [mask] + [None] * len(keys), None, None
        )

    each_head(head, 2)


def mid_kernel(n, q_ref, *refs):
    m_in, acc_in, m_out, acc_out = refs[n:]

    def head(h):
        keys, values = pieces(refs[:n])
        q = q_ref[:, head_cols(h)]
        m_out[h], acc_out[h] = absorb(q, keys, values, [None] * len(keys), m_in[h], acc_in[h])

    each_head(head)


W_BLOCK = 512


def product(rel, w, c):
    return jnp.dot(rel, w[:, pl.ds(c, W_BLOCK)], preferred_element_type=jnp.float32).astype(jnp.bfloat16)


def last_kernel(n, spot, q_ref, *refs):
    m_in, acc_in, w, rel_out, own_b, yb, ctx = refs[n:]

    def head(h):
        keys, values = pieces(refs[:n])
        q = q_ref[:, head_cols(h)]
        _, acc = absorb(q, keys, values, [None] * len(keys), m_in[h], acc_in[h])
        ctx[:, head_cols(h)] = (acc[:, :HD] / acc[:, HD:]).astype(jnp.bfloat16)

    each_head(head)

    tile = own_b.shape[1]
    half = own_b.shape[2]
    tp_of = [((spot[0] + dy) % 2) * 4 + (spot[1] + dx) % 4 for dy in range(2) for dx in range(4)]
    rel = jnp.concatenate([ctx[pl.ds(pl.multiple_of(t * tile, tile), tile)] for t in tp_of], axis=0)
    rel_out[...] = rel

    def block(i, carry):
        c = pl.multiple_of(i * W_BLOCK, W_BLOCK)
        y = product(rel_out[...], w, half + c)
        for dy, ref in enumerate((own_b, yb)):
            for dx in range(4):
                ref[dx, :, pl.ds(c, W_BLOCK)] = y[(dy * 4 + dx) * tile : (dy * 4 + dx + 1) * tile]
        return carry

    lax.fori_loop(0, half // W_BLOCK, block, 0, unroll=2)


def left_kernel(rel_ref, w, own_a, x1, x2, x3):
    tile = own_a.shape[1]

    def block(i, carry):
        c = pl.multiple_of(i * W_BLOCK, W_BLOCK)
        y = product(rel_ref[...], w, c)
        for dx, ref in enumerate((own_a, x1, x2, x3)):
            for dy in range(2):
                ref[dy, :, pl.ds(c, W_BLOCK)] = y[(dy * 4 + dx) * tile : (dy * 4 + dx + 1) * tile]
        return carry

    lax.fori_loop(0, own_a.shape[2] // W_BLOCK, block, 0, unroll=2)


VM = pl.BlockSpec(memory_space=pltpu.VMEM)
ANY = pl.BlockSpec(memory_space=pl.ANY)
SM = pl.BlockSpec(memory_space=pltpu.SMEM)


def cost(rows, keys, extra=0):
    return pl.CostEstimate(
        flops=4 * rows * HEADS * keys * HD + extra, transcendentals=rows * HEADS * keys, bytes_accessed=0
    )


def state_shapes(rows):
    return (
        jax.ShapeDtypeStruct((HEADS, rows, HD), jnp.float32),
        jax.ShapeDtypeStruct((HEADS, rows, 2 * HD), jnp.float32),
    )


def key_count(kvs):
    return sum(a.shape[0] for a in kvs) * PIECE


def windows(at):
    z, c = at[1], at[2]
    up = 1 - 2 * c
    spots = [(z * 2 * PIECE + c * PIECE, PIECE)]
    spots += [(lax.rem(z + up * d + 8, 8) * 2 * PIECE, 2 * PIECE) for d in (1, 2, 3)]
    spots.append((lax.rem(z + 4, 8) * 2 * PIECE + c * PIECE, PIECE))
    return [pl.ds(pl.multiple_of(start, PIECE), size) for start, size in spots]


def cut_kernel(at, prefix, *refs):
    outs, sem = refs[:5], refs[5]
    copies = [
        pltpu.make_async_copy(prefix.at[:, rows], ref, sem.at[i])
        for i, (rows, ref) in enumerate(zip(windows(at), outs))
    ]
    for copy in copies:
        copy.start()
    for copy in copies:
        copy.wait()


def choose_kernel(at, partner, *refs):
    mine, outs = refs[:5], refs[5:]

    @pl.when(at[0] == 1)
    def _():
        for ref, out in zip(mine, outs):
            out[...] = ref[...]

    @pl.when(at[0] == 0)
    def _():
        for rows, out in zip(windows(at), outs):
            out[...] = partner[:, rows, :]


def cut_call(kernel, at, source, *mine):
    part = lambda size: jax.ShapeDtypeStruct((2, size, HD), jnp.bfloat16)
    return pl.pallas_call(
        kernel,
        out_shape=(part(PIECE),) + (part(2 * PIECE),) * 3 + (part(PIECE),),
        in_specs=[SM] + [VM if mine else ANY] * (1 + len(mine)),
        out_specs=(VM,) * 5,
        scratch_shapes=[] if mine else [pltpu.SemaphoreType.DMA((5,))],
        compiler_params=pltpu.CompilerParams(vmem_limit_bytes=4 << 20),
        cost_estimate=pl.CostEstimate(flops=1 << 28, transcendentals=0, bytes_accessed=0),
    )(at, source, *mine)


def first_call(lens, q, ck, cv, kvs):
    rows = q.shape[0]
    return pl.pallas_call(
        first_kernel,
        out_shape=state_shapes(rows),
        in_specs=[SM] + [VM] * (3 + len(kvs)),
        out_specs=(VM, VM),
        cost_estimate=cost(rows, PIECE + key_count(kvs)),
        compiler_params=pltpu.CompilerParams(vmem_limit_bytes=12 << 20),
        name="attn_first",
    )(lens, q, ck, cv, *kvs)


def mid_call(q, kvs, state):
    n = len(kvs)
    rows = q.shape[0]
    return pl.pallas_call(
        functools.partial(mid_kernel, n),
        out_shape=state_shapes(rows),
        in_specs=[VM] * (n + 3),
        out_specs=(VM, VM),
        input_output_aliases={n + 1: 0, n + 2: 1},
        cost_estimate=cost(rows, key_count(kvs)),
        compiler_params=pltpu.CompilerParams(vmem_limit_bytes=12 << 20),
        name="attn_mid",
    )(q, *kvs, *state)


def last_call(spot, q, kvs, state, w):
    n = len(kvs)
    rows = q.shape[0]
    part = lambda k: jax.ShapeDtypeStruct((k, rows // 8, w.shape[1] // 2), jnp.bfloat16)
    outs = (jax.ShapeDtypeStruct((rows, w.shape[0]), jnp.bfloat16), part(4), part(4))
    return pl.pallas_call(
        functools.partial(last_kernel, n),
        out_shape=outs,
        in_specs=[SM] + [VM] * (n + 4),
        out_specs=(VM,) * len(outs),
        scratch_shapes=[pltpu.VMEM((rows, w.shape[0]), jnp.bfloat16)],
        cost_estimate=cost(rows, key_count(kvs), rows * w.shape[0] * w.shape[1]),
        compiler_params=pltpu.CompilerParams(vmem_limit_bytes=12 << 20),
        name="attn_last",
    )(spot, q, *kvs, *state, w)


def left_call(rel, w):
    rows = rel.shape[0]
    part = jax.ShapeDtypeStruct((2, rows // 8, w.shape[1] // 2), jnp.bfloat16)
    return pl.pallas_call(
        left_kernel,
        out_shape=(part,) * 4,
        in_specs=[VM] * 2,
        out_specs=(VM,) * 4,
        cost_estimate=pl.CostEstimate(flops=rows * w.shape[0] * w.shape[1], transcendentals=0, bytes_accessed=0),
        compiler_params=pltpu.CompilerParams(vmem_limit_bytes=12 << 20),
        name="project_left",
    )(rel, w)


def f32(a):
    return a.astype(jnp.float32)


def reduce_rows(rel, own_b, yb, w):
    over_tp = functools.partial(lax.ppermute, axis_name="tp")
    ry = over_tp(yb, perm=YLO_SWAP)
    own_a, x1, x2, x3 = left_call(rel, w)
    r2 = over_tp(x2, perm=x_shift(2))
    r1 = over_tp(x1, perm=x_shift(1))
    r3 = over_tp(x3, perm=x_shift(-1))
    u = f32(own_b) + f32(ry)
    ub = u.astype(jnp.bfloat16)
    t1 = over_tp(ub[1], perm=x_shift(1))
    t3 = over_tp(ub[3], perm=x_shift(-1))
    t2 = over_tp(ub[2], perm=x_shift(2))
    s = f32(own_a) + f32(r1) + f32(r3) + f32(r2)
    ty = over_tp(s[1].astype(jnp.bfloat16), perm=YLO_SWAP)
    left = s[0] + f32(ty)
    right = u[0] + f32(t1) + f32(t3) + f32(t2)
    return jnp.concatenate([left, right], axis=1).astype(jnp.bfloat16)


def body(queries, cand_keys, cand_values, prefix_kv, owner, lengths, out_weight):
    rep = lax.axis_index("rep")
    my_yh, my_z, my_c = rep // 16, (rep // 2) % 8, rep % 2
    tp = lax.axis_index("tp")
    spot = jnp.stack([tp // 4, tp % 4]).astype(jnp.int32)
    root = owner[0]
    root_yh, root_z, root_c = root // 16, (root // 2) % 8, root % 2
    over_rep = functools.partial(lax.ppermute, axis_name="rep")

    cut_at = jnp.stack([my_c == root_c, my_z, my_c]).astype(jnp.int32)
    steps = (my_z - root_z) % 8
    steps = jnp.where(my_c == 0, steps, (8 - steps) % 8)
    prefix = prefix_kv[0]
    cut_at, spot, steps, root_z, root_yh, my_c, my_yh = lax.optimization_barrier(
        (cut_at, spot, steps, root_z, root_yh, my_c, my_yh)
    )
    partner = over_rep(prefix, perm=CORE_SWAP)
    parts = cut_call(cut_kernel, cut_at, prefix)
    own, *outgoing = cut_call(choose_kernel, cut_at, partner, *parts)

    def branch(b):
        def send(steps, own, *parts):
            got = {}
            for d in (3, 4, 2, 1):
                roots = {1: range(b % 2, 8, 2), 2: (b % 4, b % 4 + 4)}.get(d, (b,))
                pairs = [
                    (rep_id(y, z, c), rep_id(y, z + (1 - 2 * c) * d, c))
                    for y in range(2)
                    for z in roots
                    for c in range(2)
                ]
                got[d] = over_rep(parts[d - 1], perm=pairs)
            twice = lambda a: jnp.concatenate([a, a], axis=1)
            got[4] = twice(got[4])
            return lax.select_n(jnp.minimum(steps, 4), twice(own), got[1], got[2], got[3], got[4])

        return send

    slot = lax.switch(root_z, [branch(b) for b in range(8)], steps, own, *outgoing)
    half_of = lambda a, c: lax.dynamic_slice_in_dim(a, c * PIECE, PIECE, 1)
    from_partner = over_rep(half_of(slot, 1 - my_c), perm=CORE_SWAP)
    piece = jnp.where(steps <= 4, half_of(slot, my_c), from_partner)
    across = over_rep(piece, perm=YHI_SWAP)
    a0 = jnp.where(my_yh == root_yh, piece, across)[None]

    facing = over_rep(a0, perm=z_shift(4))
    above = over_rep(a0, perm=z_shift(-1))
    below = over_rep(a0, perm=z_shift(1))
    own_other = over_rep(a0, perm=CORE_SWAP)
    state = first_call(lengths[0], queries, cand_keys, cand_values, [a0, own_other])
    above, below, facing, state = lax.optimization_barrier((above, below, facing, state))

    far_above = over_rep(jnp.concatenate([above, facing]), perm=z_shift(-1))
    far_below = over_rep(jnp.concatenate([below, facing]), perm=z_shift(1))
    near_other = over_rep(jnp.concatenate([above, below, facing]), perm=CORE_SWAP)
    state = mid_call(queries, [above, below, facing], state)
    state = mid_call(queries, [near_other], state)
    far_above, far_below, state = lax.optimization_barrier((far_above, far_below, state))

    far_other = over_rep(jnp.concatenate([far_above, far_below]), perm=CORE_SWAP)
    state = mid_call(queries, [far_above, far_below], state)
    return reduce_rows(*last_call(spot, queries, [far_other], state, out_weight), out_weight)


def solution(mesh):
    in_specs = (
        P("rep", "tp"),
        P("rep", "tp"),
        P("rep", "tp"),
        P("rep", None, None, "tp"),
        P(),
        P("rep", None),
        P("tp", None),
    )
    out_specs = P(("rep", "tp"), None)
    return jax.shard_map(body, mesh=mesh, in_specs=in_specs, out_specs=out_specs, check_vma=False)
```

```python
import functools
import math

import jax
import jax.numpy as jnp
from jax import lax
from jax.experimental import pallas as pl
from jax.experimental.pallas import tpu as pltpu
from jax.sharding import PartitionSpec as P

HEADS = 8
HD = 128
CLEN = 128
PIECE = 256
NEG = -1e30
SCALE = math.log2(math.e) / math.sqrt(HD)


REP = [(y, z, c) for y in range(2) for z in range(8) for c in range(2)]
TP = [(y, x) for y in range(2) for x in range(4)]


def rep_id(y, z, c):
    return y * 16 + (z % 8) * 2 + c


def tp_id(y, x):
    return y * 4 + x % 4


CORE_SWAP = [(rep_id(*r), rep_id(r[0], r[1], 1 - r[2])) for r in REP]
YHI_SWAP = [(rep_id(*r), rep_id(1 - r[0], r[1], r[2])) for r in REP]
YLO_SWAP = [(tp_id(y, x), tp_id(1 - y, x)) for y, x in TP]


def z_shift(d):
    return [(rep_id(y, z, c), rep_id(y, z + d, c)) for y, z, c in REP]


def x_shift(d):
    return [(tp_id(y, x), tp_id(y, x + d)) for y, x in TP]


def lanes(s):
    return [s[:, i * 128 : (i + 1) * 128] for i in range(s.shape[1] // 128)]


def absorb(q, keys, values, masks, m_old, acc_old):
    cols = []
    for k, mask in zip(keys, masks):
        s = lanes(lax.dot_general(q, k, (((1,), (1,)), ((), ())), preferred_element_type=jnp.float32))
        if mask is not None:
            s = [jnp.where(ok, t, NEG) for ok, t in zip(mask, s)]
        cols += s
    top = jnp.max(functools.reduce(jnp.maximum, cols), axis=1, keepdims=True)
    m_new = jnp.broadcast_to(top, (q.shape[0], 128)) if m_old is None else jnp.maximum(m_old, top)
    shift = m_new * SCALE
    p = jnp.concatenate([jnp.exp2(t * SCALE - shift).astype(jnp.bfloat16) for t in cols], axis=1)
    v = jnp.concatenate(values, axis=0)
    v = jnp.concatenate([v, jnp.ones(v.shape, jnp.bfloat16)], axis=1)
    pv = jnp.dot(p, v, preferred_element_type=jnp.float32)
    if m_old is None:
        return m_new, pv
    decay = jnp.exp2(m_old * SCALE - shift)
    return m_new, acc_old * jnp.concatenate([decay, decay], axis=1) + pv


def pieces(refs):
    keys = [r[j, 0] for r in refs for j in range(r.shape[0])]
    values = [r[j, 1] for r in refs for j in range(r.shape[0])]
    return keys, values


UNROLL = 8


def each_head(f, unroll=UNROLL):
    def step(i, carry):
        for j in range(unroll):
            f(i * unroll + j)
        return carry

    lax.fori_loop(0, HEADS // unroll, step, 0)


def head_cols(h):
    return pl.ds(pl.multiple_of(h * HD, HD), HD)


def first_kernel(lens, q_ref, ck, cv, *refs):
    m_out, acc_out = refs[-2:]
    rows = q_ref.shape[0]

    def head(h):
        keys, values = pieces(refs[:-2])
        slot = lax.broadcasted_iota(jnp.int32, (rows, 128), 0) // CLEN
        lane = lax.broadcasted_iota(jnp.int32, (rows, 128), 1)
        mask = [(slot == t) & (lane < lens[t]) for t in range(2)]
        q = q_ref[:, head_cols(h)]
        m_out[h], acc_out[h] = absorb(
            q, [ck[...]] + keys, [cv[...]] + values, [mask] + [None] * len(keys), None, None
        )

    each_head(head, 2)


def mid_kernel(n, q_ref, *refs):
    m_in, acc_in, m_out, acc_out = refs[n:]

    def head(h):
        keys, values = pieces(refs[:n])
        q = q_ref[:, head_cols(h)]
        m_out[h], acc_out[h] = absorb(q, keys, values, [None] * len(keys), m_in[h], acc_in[h])

    each_head(head)


W_BLOCK = 512


def product(rel, w, c):
    return jnp.dot(rel, w[:, pl.ds(c, W_BLOCK)], preferred_element_type=jnp.float32).astype(jnp.bfloat16)


def last_kernel(n, spot, q_ref, *refs):
    m_in, acc_in, w, rel_out, own_b, yb, ctx = refs[n:]

    def head(h):
        keys, values = pieces(refs[:n])
        q = q_ref[:, head_cols(h)]
        _, acc = absorb(q, keys, values, [None] * len(keys), m_in[h], acc_in[h])
        ctx[:, head_cols(h)] = (acc[:, :HD] / acc[:, HD:]).astype(jnp.bfloat16)

    each_head(head)

    tile = own_b.shape[1]
    half = own_b.shape[2]
    tp_of = [((spot[0] + dy) % 2) * 4 + (spot[1] + dx) % 4 for dy in range(2) for dx in range(4)]
    rel = jnp.concatenate([ctx[pl.ds(pl.multiple_of(t * tile, tile), tile)] for t in tp_of], axis=0)
    rel_out[...] = rel

    def block(i, carry):
        c = pl.multiple_of(i * W_BLOCK, W_BLOCK)
        y = product(rel_out[...], w, half + c)
        for dy, ref in enumerate((own_b, yb)):
            for dx in range(4):
                ref[dx, :, pl.ds(c, W_BLOCK)] = y[(dy * 4 + dx) * tile : (dy * 4 + dx + 1) * tile]
        return carry

    lax.fori_loop(0, half // W_BLOCK, block, 0, unroll=2)


def left_kernel(rel_ref, w, own_a, x1, x2, x3):
    tile = own_a.shape[1]

    def block(i, carry):
        c = pl.multiple_of(i * W_BLOCK, W_BLOCK)
        y = product(rel_ref[...], w, c)
        for dx, ref in enumerate((own_a, x1, x2, x3)):
            for dy in range(2):
                ref[dy, :, pl.ds(c, W_BLOCK)] = y[(dy * 4 + dx) * tile : (dy * 4 + dx + 1) * tile]
        return carry

    lax.fori_loop(0, own_a.shape[2] // W_BLOCK, block, 0, unroll=2)


VM = pl.BlockSpec(memory_space=pltpu.VMEM)
ANY = pl.BlockSpec(memory_space=pl.ANY)
SM = pl.BlockSpec(memory_space=pltpu.SMEM)


def cost(rows, keys, extra=0):
    return pl.CostEstimate(
        flops=4 * rows * HEADS * keys * HD + extra, transcendentals=rows * HEADS * keys, bytes_accessed=0
    )


def state_shapes(rows):
    return (
        jax.ShapeDtypeStruct((HEADS, rows, HD), jnp.float32),
        jax.ShapeDtypeStruct((HEADS, rows, 2 * HD), jnp.float32),
    )


def key_count(kvs):
    return sum(a.shape[0] for a in kvs) * PIECE


def windows(at):
    z, c = at[1], at[2]
    up = 1 - 2 * c
    ahead = lambda d: (lax.rem(z + up * d + 8, 8) * 2 * PIECE, 2 * PIECE)
    half = lambda d: (lax.rem(z + d, 8) * 2 * PIECE + c * PIECE, PIECE)
    spots = [ahead(3), half(4), ahead(2), ahead(1), half(0)]
    return [pl.ds(pl.multiple_of(start, PIECE), size) for start, size in spots]


def cut_kernel(at, prefix, *refs):
    outs, sem = refs[:5], refs[5]
    copies = [
        pltpu.make_async_copy(prefix.at[:, rows], ref, sem.at[i])
        for i, (rows, ref) in enumerate(zip(windows(at), outs))
    ]
    for copy in copies:
        copy.start()
    for copy in copies:
        copy.wait()


def choose_kernel(at, partner, *refs):
    mine, outs = refs[:5], refs[5:]

    @pl.when(at[0] == 1)
    def _():
        for ref, out in zip(mine, outs):
            out[...] = ref[...]

    @pl.when(at[0] == 0)
    def _():
        for rows, out in zip(windows(at), outs):
            out[...] = partner[:, rows, :]


def cut_call(kernel, at, source, *mine):
    part = lambda size: jax.ShapeDtypeStruct((2, size, HD), jnp.bfloat16)
    return pl.pallas_call(
        kernel,
        out_shape=tuple(part(n * PIECE) for n in (2, 1, 2, 2, 1)),
        in_specs=[SM] + [VM if mine else ANY] * (1 + len(mine)),
        out_specs=(VM,) * 5,
        scratch_shapes=[] if mine else [pltpu.SemaphoreType.DMA((5,))],
        compiler_params=pltpu.CompilerParams(vmem_limit_bytes=4 << 20),
        cost_estimate=pl.CostEstimate(flops=1 << 28, transcendentals=0, bytes_accessed=0),
    )(at, source, *mine)


def first_call(lens, q, ck, cv, kvs):
    rows = q.shape[0]
    return pl.pallas_call(
        first_kernel,
        out_shape=state_shapes(rows),
        in_specs=[SM] + [VM] * (3 + len(kvs)),
        out_specs=(VM, VM),
        cost_estimate=cost(rows, PIECE + key_count(kvs)),
        compiler_params=pltpu.CompilerParams(vmem_limit_bytes=12 << 20),
        name="attn_first",
    )(lens, q, ck, cv, *kvs)


def mid_call(q, kvs, state):
    n = len(kvs)
    rows = q.shape[0]
    return pl.pallas_call(
        functools.partial(mid_kernel, n),
        out_shape=state_shapes(rows),
        in_specs=[VM] * (n + 3),
        out_specs=(VM, VM),
        input_output_aliases={n + 1: 0, n + 2: 1},
        cost_estimate=cost(rows, key_count(kvs)),
        compiler_params=pltpu.CompilerParams(vmem_limit_bytes=12 << 20),
        name="attn_mid",
    )(q, *kvs, *state)


def last_call(spot, q, kvs, state, w):
    n = len(kvs)
    rows = q.shape[0]
    part = lambda k: jax.ShapeDtypeStruct((k, rows // 8, w.shape[1] // 2), jnp.bfloat16)
    outs = (jax.ShapeDtypeStruct((rows, w.shape[0]), jnp.bfloat16), part(4), part(4))
    return pl.pallas_call(
        functools.partial(last_kernel, n),
        out_shape=outs,
        in_specs=[SM] + [VM] * (n + 4),
        out_specs=(VM,) * len(outs),
        scratch_shapes=[pltpu.VMEM((rows, w.shape[0]), jnp.bfloat16)],
        cost_estimate=cost(rows, key_count(kvs), rows * w.shape[0] * w.shape[1]),
        compiler_params=pltpu.CompilerParams(vmem_limit_bytes=12 << 20),
        name="attn_last",
    )(spot, q, *kvs, *state, w)


def left_call(rel, w):
    rows = rel.shape[0]
    part = jax.ShapeDtypeStruct((2, rows // 8, w.shape[1] // 2), jnp.bfloat16)
    return pl.pallas_call(
        left_kernel,
        out_shape=(part,) * 4,
        in_specs=[VM] * 2,
        out_specs=(VM,) * 4,
        cost_estimate=pl.CostEstimate(flops=rows * w.shape[0] * w.shape[1], transcendentals=0, bytes_accessed=0),
        compiler_params=pltpu.CompilerParams(vmem_limit_bytes=12 << 20),
        name="project_left",
    )(rel, w)


def f32(a):
    return a.astype(jnp.float32)


def reduce_rows(rel, own_b, yb, w):
    over_tp = functools.partial(lax.ppermute, axis_name="tp")
    ry = over_tp(yb, perm=YLO_SWAP)
    own_a, x1, x2, x3 = left_call(rel, w)
    r2 = over_tp(x2, perm=x_shift(2))
    r1 = over_tp(x1, perm=x_shift(1))
    r3 = over_tp(x3, perm=x_shift(-1))
    u = f32(own_b) + f32(ry)
    ub = u.astype(jnp.bfloat16)
    t1 = over_tp(ub[1], perm=x_shift(1))
    t3 = over_tp(ub[3], perm=x_shift(-1))
    t2 = over_tp(ub[2], perm=x_shift(2))
    s = f32(own_a) + f32(r1) + f32(r3) + f32(r2)
    ty = over_tp(s[1].astype(jnp.bfloat16), perm=YLO_SWAP)
    left = s[0] + f32(ty)
    right = u[0] + f32(t1) + f32(t3) + f32(t2)
    return jnp.concatenate([left, right], axis=1).astype(jnp.bfloat16)


def body(queries, cand_keys, cand_values, prefix_kv, owner, lengths, out_weight):
    rep = lax.axis_index("rep")
    my_yh, my_z, my_c = rep // 16, (rep // 2) % 8, rep % 2
    tp = lax.axis_index("tp")
    spot = jnp.stack([tp // 4, tp % 4]).astype(jnp.int32)
    root = owner[0]
    root_yh, root_z, root_c = root // 16, (root // 2) % 8, root % 2
    over_rep = functools.partial(lax.ppermute, axis_name="rep")

    cut_at = jnp.stack([my_c == root_c, my_z, my_c]).astype(jnp.int32)
    steps = (my_z - root_z) % 8
    steps = jnp.where(my_c == 0, steps, (8 - steps) % 8)
    prefix = prefix_kv[0]
    cut_at, spot, steps, root_z, root_yh, my_c, my_yh = lax.optimization_barrier(
        (cut_at, spot, steps, root_z, root_yh, my_c, my_yh)
    )
    partner = over_rep(prefix, perm=CORE_SWAP)
    parts = cut_call(cut_kernel, cut_at, prefix)
    part_3, part_4, part_2, part_1, own = cut_call(choose_kernel, cut_at, partner, *parts)

    def branch(b):
        def send(steps, own, *parts):
            got = {}
            for d in (3, 4, 2, 1):
                roots = {1: range(b % 2, 8, 2), 2: (b % 4, b % 4 + 4)}.get(d, (b,))
                pairs = [
                    (rep_id(y, z, c), rep_id(y, z + (1 - 2 * c) * d, c))
                    for y in range(2)
                    for z in roots
                    for c in range(2)
                ]
                got[d] = over_rep(parts[d - 1], perm=pairs)
            twice = lambda a: jnp.concatenate([a, a], axis=1)
            got[4] = twice(got[4])
            return lax.select_n(jnp.minimum(steps, 4), twice(own), got[1], got[2], got[3], got[4])

        return send

    slot = lax.switch(root_z, [branch(b) for b in range(8)], steps, own, part_1, part_2, part_3, part_4)
    half_of = lambda a, c: lax.dynamic_slice_in_dim(a, c * PIECE, PIECE, 1)
    from_partner = over_rep(half_of(slot, 1 - my_c), perm=CORE_SWAP)
    piece = jnp.where(steps <= 4, half_of(slot, my_c), from_partner)
    across = over_rep(piece, perm=YHI_SWAP)
    a0 = jnp.where(my_yh == root_yh, piece, across)[None]

    facing = over_rep(a0, perm=z_shift(4))
    above = over_rep(a0, perm=z_shift(-1))
    below = over_rep(a0, perm=z_shift(1))
    own_other = over_rep(a0, perm=CORE_SWAP)
    state = first_call(lengths[0], queries, cand_keys, cand_values, [a0, own_other])
    above, below, facing, state = lax.optimization_barrier((above, below, facing, state))

    far_above = over_rep(jnp.concatenate([above, facing]), perm=z_shift(-1))
    far_below = over_rep(jnp.concatenate([below, facing]), perm=z_shift(1))
    near_other = over_rep(jnp.concatenate([above, below, facing]), perm=CORE_SWAP)
    state = mid_call(queries, [above, below, facing], state)
    state = mid_call(queries, [near_other], state)
    far_above, far_below, state = lax.optimization_barrier((far_above, far_below, state))

    far_other = over_rep(jnp.concatenate([far_above, far_below]), perm=CORE_SWAP)
    state = mid_call(queries, [far_above, far_below], state)
    return reduce_rows(*last_call(spot, queries, [far_other], state, out_weight), out_weight)


def solution(mesh):
    in_specs = (
        P("rep", "tp"),
        P("rep", "tp"),
        P("rep", "tp"),
        P("rep", None, None, "tp"),
        P(),
        P("rep", None),
        P("tp", None),
    )
    out_specs = P(("rep", "tp"), None)
    return jax.shard_map(body, mesh=mesh, in_specs=in_specs, out_specs=out_specs, check_vma=False)
```
